32 devices in a mesh: dp: 16 (over z, y, x), mp: 2 (over core).
Axes of the slice: x: 2, y: 2, z: 4, core: 2. Of those that a mesh axis runs over, the one named last changes fastest.
Arguments:
- hidden_state: bfloat16 [32, 19, 19, 256], P('dp'), may hold values from -6 to 6
- actions: int32 [32, 2], P('dp'), may hold values from 0 to 361
- value_target: int32 [32, 2], P('dp'), may hold values from 0 to 600
- reward_target: int32 [32, 2], P('dp'), may hold values from 0 to 600
- kernel_first: float32 [3, 3, 256, 256], P(None, None, 'dp', 'mp'), may hold values from -6 to 6
- kernel_second: float32 [3, 3, 256, 256], P(None, None, 'dp', 'mp'), may hold values from -6 to 6
- head_weight: float32 [2, 256, 601], P('mp', 'dp'), may hold values from -6 to 6
- action_embed: float32 [2, 256], P('mp', 'dp'), may hold values from -6 to 6
- first_mean: float32 [3, 3, 256, 256], P(None, None, 'dp', 'mp'), may hold values from -0.00061035156 to 0.00061035156
- first_square: float32 [3, 3, 256, 256], P(None, None, 'dp', 'mp'), may hold values from 1e-09 to 1e-06
- second_mean: float32 [3, 3, 256, 256], P(None, None, 'dp', 'mp'), may hold values from -0.00061035156 to 0.00061035156
- second_square: float32 [3, 3, 256, 256], P(None, None, 'dp', 'mp'), may hold values from 1e-09 to 1e-06
- head_mean: float32 [2, 256, 601], P('mp', 'dp'), may hold values from -0.0029296875 to 0.0029296875
- head_square: float32 [2, 256, 601], P('mp', 'dp'), may hold values from 1e-08 to 1e-06
- embed_mean: float32 [2, 256], P('mp', 'dp'), may hold values from -0.0017089844 to 0.0017089844
- embed_square: float32 [2, 256], P('mp', 'dp'), may hold values from 1e-09 to 1e-06
Outputs:
- kernel_first_new: float32 [3, 3, 256, 256], P(None, None, 'dp', 'mp')
- kernel_second_new: float32 [3, 3, 256, 256], P(None, None, 'dp', 'mp')
- head_weight_new: float32 [2, 256, 601], P('mp', 'dp')
- action_embed_new: float32 [2, 256], P('mp', 'dp')
- first_mean_new: float32 [3, 3, 256, 256], P(None, None, 'dp', 'mp')
- first_square_new: float32 [3, 3, 256, 256], P(None, None, 'dp', 'mp')
- second_mean_new: float32 [3, 3, 256, 256], P(None, None, 'dp', 'mp')
- second_square_new: float32 [3, 3, 256, 256], P(None, None, 'dp', 'mp')
- head_mean_new: float32 [2, 256, 601], P('mp', 'dp')
- head_square_new: float32 [2, 256, 601], P('mp', 'dp')
- embed_mean_new: float32 [2, 256], P('mp', 'dp')
- embed_square_new: float32 [2, 256], P('mp', 'dp')
- first_grad: float32 [3, 3, 256, 256], P(None, None, 'dp', 'mp')
- second_grad: float32 [3, 3, 256, 256], P(None, None, 'dp', 'mp')
- head_grad: float32 [2, 256, 601], P('mp', 'dp')
- embed_grad: float32 [2, 256], P('mp', 'dp')
The draws below stay inside these ranges and needn't reach their ends.
Inputs may be any that keep to these rules, and one draw needn't show every extreme that they name: `actions`: the value 361 stands for a pass.
All inputs are finite; a program needn't handle non-finite values.
Results may differ from the reference program's by a relative error of at most 0.02.
Values may be sent and summed in bfloat16 or wider, within the bound.
No kernel may reach another device: no remote copies, remote signals or barrier semaphores. Data moves between devices by JAX's collectives and lax.ppermute only.
A program may use at most 64 MiB of HBM per device.

```python
import math
import jax
import jax.numpy as jnp
from jax import lax

CHANNELS = 256
BOARD = 19
CELLS = 361
BUCKETS = 601
UNROLL = 2
TOTAL_POS = 32


def touch_ends(entries, stream_key, least, top_value):
    extent = entries.shape
    spot = [jax.random.randint(jax.random.fold_in(stream_key, axis), (), 0, extent[axis]) for axis in range(len(extent))]
    entries = entries.at[tuple(spot)].set(least)
    longest = extent.index(max(extent))
    spot[longest] = (spot[longest] + 1) % extent[longest]
    return entries.at[tuple(spot)].set(top_value)


def shard_levels(rng, shape, split, smallest, high):
    loudness, own = 1.0, jax.random.fold_in(rng, 6)
    for axis_at, shards_of in split:
        draws = jnp.exp(jax.random.uniform(jax.random.fold_in(own, axis_at), (shards_of,), jnp.float32, smallest / len(split), high / len(split)))
        loudness = loudness * jnp.repeat(draws, shape[axis_at] // shards_of).reshape([-1 if axis == axis_at else 1 for axis in range(len(shape))])
    return loudness


def noise(key, extent, scale, most, cuts=(), held_as=jnp.bfloat16):
    loudness = shard_levels(key, extent, cuts, -0.22, 0.18) if cuts else 1.0
    drawn = jax.random.normal(key, extent, jnp.float32) * scale * loudness
    return jnp.minimum(jnp.maximum(drawn, -most), most).astype(held_as)


def setup_inputs(seed: int = 0) -> dict:
    keys = jax.random.split(jax.random.key(seed), 17)
    return {
        "hidden_state": noise(keys[0], (TOTAL_POS, BOARD, BOARD, CHANNELS), 1.0, 6.0, ((0, 16),)),
        "actions": touch_ends(jax.random.randint(keys[1], (TOTAL_POS, UNROLL), 0, CELLS + 1), jax.random.fold_in(keys[1], 1), 0, CELLS).astype(jnp.int32),
        "value_target": touch_ends(jax.random.randint(keys[2], (TOTAL_POS, UNROLL), 0, BUCKETS), jax.random.fold_in(keys[2], 1), 0, BUCKETS - 1).astype(jnp.int32),
        "reward_target": touch_ends(jax.random.randint(keys[3], (TOTAL_POS, UNROLL), 0, BUCKETS), jax.random.fold_in(keys[3], 1), 0, BUCKETS - 1).astype(jnp.int32),
        "kernel_first": noise(keys[4], (3, 3, CHANNELS, CHANNELS), 1.0, 6.0, ((2, 16), (3, 2)), jnp.float32),
        "kernel_second": noise(keys[5], (3, 3, CHANNELS, CHANNELS), 1.0, 6.0, ((2, 16), (3, 2)), jnp.float32),
        "head_weight": noise(keys[6], (2, CHANNELS, BUCKETS), 1.0, 6.0, ((0, 2), (1, 16)), jnp.float32),
        "action_embed": noise(keys[7], (2, CHANNELS), 1.0, 6.0, ((0, 2), (1, 16)), jnp.float32),
        "first_mean": noise(keys[8], (3, 3, CHANNELS, CHANNELS), (1e-4), 0.00061035156, ((2, 16), (3, 2)), jnp.float32),
        "first_square": jnp.clip(jnp.exp(math.log(9.999999974752427e-07) - 6.9077553 * jax.random.uniform(keys[9], (3, 3, CHANNELS, CHANNELS), jnp.float32) ** shard_levels(keys[9], (3, 3, CHANNELS, CHANNELS), ((2, 16), (3, 2)), -0.2, 0.2)), 9.999999717180685e-10, 9.999999974752427e-07),
        "second_mean": noise(keys[10], (3, 3, CHANNELS, CHANNELS), (1e-4), 0.00061035156, ((2, 16), (3, 2)), jnp.float32),
        "second_square": jnp.clip(jnp.exp(math.log(9.999999974752427e-07) - 6.9077553 * jax.random.uniform(keys[11], (3, 3, CHANNELS, CHANNELS), jnp.float32) ** shard_levels(keys[11], (3, 3, CHANNELS, CHANNELS), ((2, 16), (3, 2)), -0.2, 0.2)), 9.999999717180685e-10, 9.999999974752427e-07),
        "head_mean": noise(keys[12], (2, CHANNELS, BUCKETS), (5e-4), 0.0029296875, ((0, 2), (1, 16)), jnp.float32),
        "head_square": jnp.clip(jnp.exp(math.log(9.999999974752427e-07) - 4.6051702 * jax.random.uniform(keys[13], (2, CHANNELS, BUCKETS), jnp.float32) ** shard_levels(keys[13], (2, CHANNELS, BUCKETS), ((0, 2), (1, 16)), -0.2, 0.2)), 9.99999993922529e-09, 9.999999974752427e-07),
        "embed_mean": noise(keys[14], (2, CHANNELS), (3e-4), 0.0017089844, ((0, 2), (1, 16)), jnp.float32),
        "embed_square": jnp.clip(jnp.exp(math.log(9.999999974752427e-07) - 6.9077553 * jax.random.uniform(keys[15], (2, CHANNELS), jnp.float32) ** shard_levels(keys[15], (2, CHANNELS), ((0, 2), (1, 16)), -0.2, 0.2)), 9.999999717180685e-10, 9.999999974752427e-07),
    }


head_scale = 4.0
soft_cap = 15.0
eps_norm = 1e-05
beta_one = 0.9
beta_two = 0.999
step_size = 0.1
eps_adam = 1e-08

def conv_apply(field, kernel, layout):
    return lax.conv_general_dilated(field, kernel, (1, 1), 'SAME', dimension_numbers=('NHWC', layout, 'NHWC'), preferred_element_type=jnp.float32)

def gate_slope(pre):
    sig = jax.nn.sigmoid(pre)
    return sig * (1.0 + pre * (1.0 - sig))

def tap_products(field, grad, field_rows):
    side = field.shape[1]
    padded = jnp.pad(field, ((0, 0), (1, 1), (1, 1), (0, 0)))
    flat_grad = grad.reshape(-1, grad.shape[3])
    blocks = []
    for offset in range(9):
        row_start = offset // 3
        col_start = offset % 3
        window = padded[:, row_start:row_start + side, col_start:col_start + side, :].reshape(-1, field.shape[3])
        if field_rows:
            blocks.append(lax.dot_general(window, flat_grad, (((0,), (0,)), ((), ())), preferred_element_type=jnp.float32))
        else:
            blocks.append(lax.dot_general(flat_grad, window, (((0,), (0,)), ((), ())), preferred_element_type=jnp.float32))
    stacked = jnp.stack(blocks)
    return stacked.reshape(3, 3, stacked.shape[1], stacked.shape[2])

def action_planes(move, board):
    cells = board * board
    plane = (lax.broadcasted_iota(jnp.int32, (move.shape[0], cells), 1) == move[:, None]).astype(jnp.float32)
    passed = (move == cells).astype(jnp.float32)
    return (plane.reshape(move.shape[0], board, board, 1), passed[:, None, None, None])

def head_backward(state, head_used, value_now, reward_now, total):
    pooled = lax.optimization_barrier(jnp.mean(state, axis=(1, 2))).astype(jnp.bfloat16)
    raw = head_scale * jnp.stack([jnp.dot(pooled, head_used[0], preferred_element_type=jnp.float32), jnp.dot(pooled, head_used[1], preferred_element_type=jnp.float32)])
    squashed = jnp.tanh(raw / soft_cap)
    raised = jnp.exp(soft_cap * squashed)
    chances = raised / lax.optimization_barrier(jnp.sum(raised, axis=2, keepdims=True))
    targets = jnp.stack([value_now, reward_now])
    picked = (lax.broadcasted_iota(jnp.int32, raw.shape, 2) == targets[:, :, None]).astype(jnp.float32)
    logit_grad = ((chances - picked) * (1.0 - squashed * squashed) / total).astype(jnp.bfloat16)
    pooled_grad = head_scale * (jnp.dot(logit_grad[0], head_used[0].T, preferred_element_type=jnp.float32) + jnp.dot(logit_grad[1], head_used[1].T, preferred_element_type=jnp.float32))
    return (pooled, logit_grad, pooled_grad)

def adam_update(param, grad, mean, square):
    mean_new = beta_one * mean + (1.0 - beta_one) * grad
    square_new = beta_two * square + (1.0 - beta_two) * grad * grad
    param_new = param - step_size * mean_new / (jnp.sqrt(square_new) + eps_adam)
    return (param_new, mean_new, square_new)

def reference(hidden_state, actions, value_target, reward_target, kernel_first, kernel_second, head_weight, action_embed, first_mean, first_square, second_mean, second_square, head_mean, head_square, embed_mean, embed_square):
    first_used = kernel_first.astype(jnp.bfloat16)
    second_used = kernel_second.astype(jnp.bfloat16)
    head_used = head_weight.astype(jnp.bfloat16)
    embed_used = action_embed.astype(jnp.bfloat16)
    board = hidden_state.shape[1]
    cells = board * board
    scale = (9.0 * CHANNELS) ** (-0.5)
    embed = embed_used.astype(jnp.float32)
    state = hidden_state.astype(jnp.float32)
    saved = []
    for position in range(UNROLL):
        plane, passed = action_planes(actions[:, position], board)
        mixed = state + plane * embed[0] + passed * embed[1]
        conv_input = mixed.astype(jnp.bfloat16)
        pre = scale * conv_apply(conv_input, first_used, 'HWIO')
        hidden = jax.nn.silu(pre).astype(jnp.bfloat16)
        summed = mixed + scale * conv_apply(hidden, second_used, 'HWOI')
        factor = lax.rsqrt(lax.optimization_barrier(jnp.mean(summed * summed, axis=(1, 2, 3), keepdims=True)) + eps_norm)
        state = summed * factor
        pooled, logit_grad, pooled_grad = head_backward(state, head_used, value_target[:, position], reward_target[:, position], TOTAL_POS)
        saved.append((plane, passed, conv_input, pre, hidden, summed, factor, pooled, logit_grad, pooled_grad))
    first_grad = jnp.zeros(kernel_first.shape, jnp.float32)
    second_grad = jnp.zeros(kernel_second.shape, jnp.float32)
    head_grad = jnp.zeros(head_weight.shape, jnp.float32)
    embed_grad = jnp.zeros(action_embed.shape, jnp.float32)
    carry = jnp.zeros(hidden_state.shape, jnp.float32)
    for position in range(UNROLL - 1, -1, -1):
        plane, passed, conv_input, pre, hidden, summed, factor, pooled, logit_grad, pooled_grad = saved[position]
        state_grad = carry + pooled_grad[:, None, None, :] / cells
        summed_grad = factor * state_grad - factor * factor * factor * summed * lax.optimization_barrier(jnp.mean(state_grad * summed, axis=(1, 2, 3), keepdims=True))
        branch_grad = summed_grad.astype(jnp.bfloat16)
        hidden_grad = scale * conv_apply(branch_grad, second_used[::-1, ::-1], 'HWIO')
        inner_grad = (hidden_grad * gate_slope(pre)).astype(jnp.bfloat16)
        carry = summed_grad + scale * conv_apply(inner_grad, first_used[::-1, ::-1], 'HWOI')
        first_grad = first_grad + scale * tap_products(conv_input, inner_grad, True)
        second_grad = second_grad + scale * tap_products(hidden, branch_grad, False)
        head_grad = head_grad + head_scale * jnp.stack([lax.dot_general(pooled, logit_grad[0], (((0,), (0,)), ((), ())), preferred_element_type=jnp.float32), lax.dot_general(pooled, logit_grad[1], (((0,), (0,)), ((), ())), preferred_element_type=jnp.float32)])
        embed_grad = embed_grad + jnp.stack([lax.optimization_barrier(jnp.sum(plane * carry, axis=(0, 1, 2))), lax.optimization_barrier(jnp.sum(passed * carry, axis=(0, 1, 2)))])
    first_new, first_mean_new, first_square_new = adam_update(kernel_first, first_grad, first_mean, first_square)
    second_new, second_mean_new, second_square_new = adam_update(kernel_second, second_grad, second_mean, second_square)
    head_new, head_mean_new, head_square_new = adam_update(head_weight, head_grad, head_mean, head_square)
    embed_new, embed_mean_new, embed_square_new = adam_update(action_embed, embed_grad, embed_mean, embed_square)
    return (first_new, second_new, head_new, embed_new, first_mean_new, first_square_new, second_mean_new, second_square_new, head_mean_new, head_square_new, embed_mean_new, embed_square_new, first_grad, second_grad, head_grad, embed_grad)
```

```python
import functools

import jax
import jax.numpy as jnp
from jax import lax
from jax.experimental import pallas as pl
from jax.experimental.pallas import tpu as pltpu
from jax.sharding import PartitionSpec as P

CHANNELS = 256
LANES = 128
TILE = 16


head_scale = 4.0
soft_cap = 15.0
eps_norm = 1e-05
beta_one = 0.9
beta_two = 0.999
step_size = 0.1
eps_adam = 1e-08


def adam_update(param, grad, mean, square):
    mean_new = beta_one * mean + (1.0 - beta_one) * grad
    square_new = beta_two * square + (1.0 - beta_two) * grad * grad
    param_new = param - step_size * mean_new / (jnp.sqrt(square_new) + eps_adam)
    return (param_new, mean_new, square_new)


def round_up(value, step):
    return -(-value // step) * step


def spread(block, axis):
    copies = jnp.broadcast_to(block[None], (lax.axis_size(axis),) + block.shape)
    return lax.all_to_all(copies, axis, 0, 0)


def row_pad(block, axis):
    short = -block.shape[axis] % TILE
    if not short:
        return block
    widths = [(0, 0)] * block.ndim
    widths[axis] = (0, short)
    return jnp.pad(block, widths)


def gather_weights(kernel_first, kernel_second, head_weight, action_embed):
    rows = kernel_first.shape[2]
    buckets = head_weight.shape[2]
    blocks = round_up(buckets, LANES) // LANES
    head = jnp.pad(head_weight[0], ((0, 0), (0, blocks * LANES - buckets)))
    head = head.reshape(rows, blocks, LANES).transpose(1, 0, 2)
    embed = jnp.pad(action_embed, ((0, TILE - 1), (0, LANES - rows)))
    packed = jnp.concatenate(
        [
            row_pad(kernel_first.astype(jnp.bfloat16).reshape(-1, LANES), 0),
            row_pad(kernel_second.astype(jnp.bfloat16).reshape(-1, LANES), 0),
            row_pad(head.astype(jnp.bfloat16).reshape(-1, LANES), 0),
            embed.astype(jnp.bfloat16),
        ]
    )
    everything = spread(spread(packed, "dp"), "mp")
    embed_used = everything[:, :, -TILE, :rows].reshape(everything.shape[0], CHANNELS)
    if rows != TILE:
        everything = regroup(everything, rows, blocks)
    return (everything, embed_used.astype(jnp.float32))


def regroup(everything, rows, blocks):
    cores, shards = everything.shape[:2]
    groups = CHANNELS // TILE
    parts = []
    begin = 0
    for taps in (9, 9, blocks):
        part = everything[:, :, begin : begin + taps * rows]
        begin += round_up(taps * rows, TILE)
        part = part.reshape(cores, groups, shards // groups, taps, rows, LANES)
        parts.append(part.transpose(0, 1, 3, 2, 4, 5).reshape(cores, groups, taps * TILE, LANES))
    parts.append(jnp.zeros((cores, groups, TILE, LANES), everything.dtype))
    return jnp.concatenate(parts, axis=2)


def ungroup(packed, rows, blocks, shards):
    cores, groups = packed.shape[:2]
    parts = []
    begin = 0
    for taps in (9, 9, blocks):
        part = packed[:, :, begin : begin + taps * TILE]
        begin += taps * TILE
        part = part.reshape(cores, groups, taps, shards // groups, rows, LANES)
        part = part.transpose(0, 1, 3, 2, 4, 5).reshape(cores, shards, taps * rows, LANES)
        parts.append(row_pad(part, 2))
    parts.append(jnp.repeat(packed[:, :, begin:], shards // groups, axis=1))
    return jnp.concatenate(parts, axis=2)


def scatter_grads(packed, rows, buckets):
    blocks = round_up(buckets, LANES) // LANES
    shards = lax.axis_size("dp")
    if rows != TILE:
        packed = ungroup(packed, rows, blocks, shards)
    halves = lax.all_to_all(packed, "mp", 0, 0)
    summed = jnp.sum(halves.astype(jnp.float32), axis=0).astype(jnp.bfloat16)
    owned = lax.all_to_all(summed, "dp", 0, 0)
    total = jnp.sum(owned.astype(jnp.float32), axis=0)
    step = round_up(9 * rows, TILE)
    first = total[: 9 * rows].reshape(3, 3, rows, LANES)
    second = total[step : step + 9 * rows].reshape(3, 3, rows, LANES)
    head = total[2 * step : 2 * step + blocks * rows].reshape(blocks, rows, LANES)
    head = head.transpose(1, 0, 2).reshape(1, rows, blocks * LANES)[:, :, :buckets]
    embed = total[-TILE : CHANNELS // LANES - TILE].reshape(1, CHANNELS)
    embed = lax.dynamic_slice_in_dim(embed, lax.axis_index("dp") * rows, rows, 1)
    return (first, second, head, embed)


def nn(left, right):
    return jnp.dot(left, right, preferred_element_type=jnp.float32)


def nt(left, right):
    return lax.dot_general(left, right, (((1,), (1,)), ((), ())), preferred_element_type=jnp.float32)


def tn(left, right):
    return lax.dot_general(left, right, (((0,), (0,)), ((), ())), preferred_element_type=jnp.float32)


def window_kernel(
    spots,
    passes,
    values,
    rewards,
    every,
    states,
    mask,
    embed,
    out,
    first,
    second,
    head,
    padded,
    fields,
    hiddens,
    taps,
    pres,
    sums,
    inners,
    branches,
    *,
    count,
    unroll,
    board,
    width,
    extent,
    buckets,
    blocks,
    total,
):
    cells = board * board
    base = 8
    scale = (9.0 * CHANNELS) ** (-0.5)
    cores = CHANNELS // LANES
    groups = CHANNELS // TILE
    spread_cols = blocks * LANES
    for core in range(cores):
        lanes = slice(core * LANES, (core + 1) * LANES)
        for group in range(groups):
            rows = slice(group * TILE, (group + 1) * TILE)
            for tap in range(9):
                at = tap * CHANNELS + group * TILE
                first[at : at + TILE, lanes] = every[core, group, tap * TILE : (tap + 1) * TILE, :]
                two = (9 + tap) * TILE
                second[at : at + TILE, lanes] = every[core, group, two : two + TILE, :]
    for which in range(2):
        for group in range(groups):
            for block in range(blocks):
                at = (18 + block) * TILE
                head[
                    which, group * TILE : (group + 1) * TILE, block * LANES : (block + 1) * LANES
                ] = every[which, group, at : at + TILE, :]
    padded[...] = jnp.zeros(padded.shape, jnp.float32)
    inside = jnp.broadcast_to(mask[...], (extent, CHANNELS)) > 0.5
    cell_at = lax.broadcasted_iota(jnp.int32, (extent, CHANNELS), 0)
    lane_at = lax.broadcasted_iota(jnp.int32, (8, spread_cols), 1)
    row_at = lax.broadcasted_iota(jnp.int32, (TILE, 1), 0)

    def lay_out(field, target, begin, flip):
        padded[base + width : base + width + extent, :] = field
        for tap in range(9):
            start = base + (tap // 3) * width + tap % 3 - 1
            slot = 8 - tap if flip else tap
            target[begin : begin + extent, slot * CHANNELS : (slot + 1) * CHANNELS] = padded[
                start : start + extent, :
            ].astype(jnp.bfloat16)

    def taps_nt(source, begin, kernel):
        result = None
        for tap in range(9):
            cols = slice(tap * CHANNELS, (tap + 1) * CHANNELS)
            part = nt(source[begin : begin + extent, cols], kernel[cols, :])
            result = part if result is None else result + part
        return result

    def grand(block):
        return jnp.sum(jnp.sum(block, axis=0, keepdims=True), axis=1, keepdims=True)

    pooled_rows = jnp.zeros((TILE, CHANNELS), jnp.float32)
    grad_rows = [jnp.zeros((TILE, spread_cols), jnp.float32) for _ in range(2)]
    factors = {}
    pulls = {}
    for n in range(count):
        state = states[n].astype(jnp.float32)
        for k in range(unroll):
            slot = k * count + n
            begin = slot * extent
            plane = cell_at == spots[n, k]
            extra = jnp.where(inside, passes[n, k].astype(jnp.float32) * embed[1:2, :], 0.0)
            mixed = state + jnp.where(plane, embed[0:1, :], 0.0) + extra
            lay_out(mixed, fields, begin, False)
            pre = scale * nn(fields[begin : begin + extent, :], first[...])
            pres[slot] = pre
            hidden = jnp.where(inside, pre * jax.nn.sigmoid(pre), 0.0)
            lay_out(hidden, hiddens, begin, False)
            branch = taps_nt(hiddens, begin, second)
            summed = jnp.where(inside, mixed + scale * branch, 0.0)
            sums[slot] = summed
            factor = lax.rsqrt(grand(summed * summed) / (cells * CHANNELS) + eps_norm)
            factors[slot] = factor
            state = summed * factor
            pooled = (jnp.sum(state, axis=0, keepdims=True) / cells).astype(jnp.bfloat16)
            pooled_rows = jnp.where(row_at == slot, pooled.astype(jnp.float32), pooled_rows)
            eight = jnp.broadcast_to(pooled.astype(jnp.float32), (8, CHANNELS)).astype(jnp.bfloat16)
            pull = jnp.zeros((8, CHANNELS), jnp.float32)
            for which, targets in enumerate((values, rewards)):
                raw = head_scale * nn(eight, head[which])
                squashed = jnp.tanh(raw / soft_cap)
                raised = jnp.where(lane_at < buckets, jnp.exp(soft_cap * squashed), 0.0)
                chances = raised / jnp.sum(raised, axis=1, keepdims=True)
                picked = jnp.where(lane_at == targets[n, k], 1.0, 0.0)
                logit_grad = (chances - picked) * (1.0 - squashed * squashed) / total
                rounded = logit_grad.astype(jnp.bfloat16)
                grad_rows[which] = jnp.where(
                    row_at == slot, rounded.astype(jnp.float32)[0:1, :], grad_rows[which]
                )
                pull = pull + nt(rounded, head[which])
            pulls[slot] = head_scale * pull[0:1, :]
    embed_grads = [jnp.zeros((1, CHANNELS), jnp.float32) for _ in range(2)]
    for n in range(count):
        carry = jnp.zeros((extent, CHANNELS), jnp.float32)
        for k in range(unroll - 1, -1, -1):
            slot = k * count + n
            begin = slot * extent
            factor = factors[slot]
            summed = sums[slot]
            state_grad = carry + jnp.where(inside, pulls[slot] / cells, 0.0)
            shared = grand(state_grad * summed) / (cells * CHANNELS)
            summed_grad = factor * state_grad - factor * factor * factor * summed * shared
            branches[begin : begin + extent, :] = summed_grad.astype(jnp.bfloat16)
            lay_out(summed_grad, taps, 0, True)
            hidden_grad = scale * nn(taps[...], second[...])
            pre = pres[slot]
            sig = jax.nn.sigmoid(pre)
            inner = jnp.where(inside, hidden_grad * (sig * (1.0 + pre * (1.0 - sig))), 0.0)
            inners[begin : begin + extent, :] = inner.astype(jnp.bfloat16)
            lay_out(inner, taps, 0, True)
            carry = jnp.where(inside, summed_grad + scale * taps_nt(taps, 0, first), 0.0)
            embed_grads[0] = embed_grads[0] + jnp.sum(
                jnp.where(cell_at == spots[n, k], carry, 0.0), axis=0, keepdims=True
            )
            embed_grads[1] = embed_grads[1] + passes[n, k].astype(jnp.float32) * jnp.sum(
                carry, axis=0, keepdims=True
            )
    turned_inner = inners[...].T
    turned_branch = branches[...].T
    for tap in range(9):
        cols = slice(tap * CHANNELS, (tap + 1) * CHANNELS)
        one = (scale * nn(turned_inner, fields[:, cols])).T.astype(jnp.bfloat16)
        two = (scale * nn(turned_branch, hiddens[:, cols])).astype(jnp.bfloat16)
        for core in range(cores):
            lanes = slice(core * LANES, (core + 1) * LANES)
            for group in range(groups):
                rows = slice(group * TILE, (group + 1) * TILE)
                out[core, group, tap * TILE : (tap + 1) * TILE, :] = one[rows, lanes]
                out[core, group, (9 + tap) * TILE : (10 + tap) * TILE, :] = two[rows, lanes]
    pooled_bf = pooled_rows.astype(jnp.bfloat16)
    for which in range(2):
        grown = head_scale * tn(pooled_bf, grad_rows[which].astype(jnp.bfloat16))
        grown = grown.astype(jnp.bfloat16)
        line = jnp.where(
            row_at == 0,
            embed_grads[which][:, :LANES],
            jnp.where(row_at == 1, embed_grads[which][:, LANES:], 0.0),
        ).astype(jnp.bfloat16)
        for group in range(groups):
            rows = slice(group * TILE, (group + 1) * TILE)
            for block in range(blocks):
                at = (18 + block) * TILE
                out[which, group, at : at + TILE, :] = grown[
                    rows, block * LANES : (block + 1) * LANES
                ]
            at = (18 + blocks) * TILE
            out[which, group, at : at + TILE, :] = line


def window(every, embed, states, moves, values, rewards, buckets, total):
    count, board = states.shape[:2]
    unroll = moves.shape[1]
    cells = board * board
    width = round_up(board + 1, 8)
    extent = round_up(board * width, TILE)
    blocks = round_up(buckets, LANES) // LANES
    states = jnp.pad(states, ((0, 0), (0, 0), (0, width - board), (0, 0)))
    states = states.reshape(count, board * width, CHANNELS)
    states = jnp.pad(states, ((0, 0), (0, extent - board * width), (0, 0)))
    passes = (moves == cells).astype(jnp.int32)
    spots = jnp.where(moves == cells, -1, moves // board * width + moves % board)
    at = jnp.arange(extent)
    mask = ((at % width < board) & (at // width < board)).astype(jnp.float32)[:, None]
    deep = count * unroll * extent
    body = functools.partial(
        window_kernel,
        count=count,
        unroll=unroll,
        board=board,
        width=width,
        extent=extent,
        buckets=buckets,
        blocks=blocks,
        total=total,
    )
    smem = pl.BlockSpec(memory_space=pltpu.SMEM)
    vmem = pl.BlockSpec(memory_space=pltpu.VMEM)
    return pl.pallas_call(
        body,
        out_shape=jax.ShapeDtypeStruct(every.shape, jnp.bfloat16),
        in_specs=[smem] * 4 + [vmem] * 4,
        out_specs=vmem,
        scratch_shapes=[
            pltpu.VMEM((9 * CHANNELS, CHANNELS), jnp.bfloat16),
            pltpu.VMEM((9 * CHANNELS, CHANNELS), jnp.bfloat16),
            pltpu.VMEM((2, CHANNELS, blocks * LANES), jnp.bfloat16),
            pltpu.VMEM((extent + 2 * width + 16, CHANNELS), jnp.float32),
            pltpu.VMEM((deep, 9 * CHANNELS), jnp.bfloat16),
            pltpu.VMEM((deep, 9 * CHANNELS), jnp.bfloat16),
            pltpu.VMEM((extent, 9 * CHANNELS), jnp.bfloat16),
            pltpu.VMEM((count * unroll, extent, CHANNELS), jnp.float32),
            pltpu.VMEM((count * unroll, extent, CHANNELS), jnp.float32),
            pltpu.VMEM((deep, CHANNELS), jnp.bfloat16),
            pltpu.VMEM((deep, CHANNELS), jnp.bfloat16),
        ],
        compiler_params=pltpu.CompilerParams(vmem_limit_bytes=56 * 1024 * 1024),
    )(spots, passes, values, rewards, every, states, mask, embed)


def local(
    hidden_state,
    actions,
    value_target,
    reward_target,
    kernel_first,
    kernel_second,
    head_weight,
    action_embed,
    first_mean,
    first_square,
    second_mean,
    second_square,
    head_mean,
    head_square,
    embed_mean,
    embed_square,
):
    total = hidden_state.shape[0] * lax.axis_size("dp")
    rows = kernel_first.shape[2]
    buckets = head_weight.shape[2]
    every, embed = gather_weights(kernel_first, kernel_second, head_weight, action_embed)
    count = hidden_state.shape[0] // lax.axis_size("mp")
    begin = lax.axis_index("mp") * count
    states = lax.dynamic_slice_in_dim(hidden_state, begin, count, 0)
    moves = lax.dynamic_slice_in_dim(actions, begin, count, 0)
    values = lax.dynamic_slice_in_dim(value_target, begin, count, 0)
    rewards = lax.dynamic_slice_in_dim(reward_target, begin, count, 0)
    packed = window(every, embed, states, moves, values, rewards, buckets, total)
    first_grad, second_grad, head_grad, embed_grad = scatter_grads(packed, rows, buckets)
    first_new, first_mean_new, first_square_new = adam_update(
        kernel_first, first_grad, first_mean, first_square
    )
    second_new, second_mean_new, second_square_new = adam_update(
        kernel_second, second_grad, second_mean, second_square
    )
    head_new, head_mean_new, head_square_new = adam_update(
        head_weight, head_grad, head_mean, head_square
    )
    embed_new, embed_mean_new, embed_square_new = adam_update(
        action_embed, embed_grad, embed_mean, embed_square
    )
    return (
        first_new,
        second_new,
        head_new,
        embed_new,
        first_mean_new,
        first_square_new,
        second_mean_new,
        second_square_new,
        head_mean_new,
        head_square_new,
        embed_mean_new,
        embed_square_new,
        first_grad,
        second_grad,
        head_grad,
        embed_grad,
    )


def solution(mesh):
    placed = (
        P("dp", None, None, None),
        P("dp", None),
        P("dp", None),
        P("dp", None),
        P(None, None, "dp", "mp"),
        P(None, None, "dp", "mp"),
        P("mp", "dp", None),
        P("mp", "dp"),
        P(None, None, "dp", "mp"),
        P(None, None, "dp", "mp"),
        P(None, None, "dp", "mp"),
        P(None, None, "dp", "mp"),
        P("mp", "dp", None),
        P("mp", "dp", None),
        P("mp", "dp"),
        P("mp", "dp"),
    )
    return jax.shard_map(
        local,
        mesh=mesh,
        in_specs=placed,
        out_specs=(
            P(None, None, "dp", "mp"),
            P(None, None, "dp", "mp"),
            P("mp", "dp", None),
            P("mp", "dp"),
            P(None, None, "dp", "mp"),
            P(None, None, "dp", "mp"),
            P(None, None, "dp", "mp"),
            P(None, None, "dp", "mp"),
            P("mp", "dp", None),
            P("mp", "dp", None),
            P("mp", "dp"),
            P("mp", "dp"),
            P(None, None, "dp", "mp"),
            P(None, None, "dp", "mp"),
            P("mp", "dp", None),
            P("mp", "dp"),
        ),
        check_vma=False,
    )
```

```python
import functools

import jax
import jax.numpy as jnp
from jax import lax
from jax.experimental import pallas as pl
from jax.experimental.pallas import tpu as pltpu
from jax.sharding import PartitionSpec as P

CHANNELS = 256
LANES = 128
TILE = 16


head_scale = 4.0
soft_cap = 15.0
eps_norm = 1e-05
beta_one = 0.9
beta_two = 0.999
step_size = 0.1
eps_adam = 1e-08


def adam_update(param, grad, mean, square):
    mean_new = beta_one * mean + (1.0 - beta_one) * grad
    square_new = beta_two * square + (1.0 - beta_two) * grad * grad
    param_new = param - step_size * mean_new / (jnp.sqrt(square_new) + eps_adam)
    return (param_new, mean_new, square_new)


def round_up(value, step):
    return -(-value // step) * step


def spread(block, axis):
    copies = jnp.broadcast_to(block[None], (lax.axis_size(axis),) + block.shape)
    return lax.all_to_all(copies, axis, 0, 0)


def swap_cores(block):
    return lax.ppermute(block, "mp", [(0, 1), (1, 0)])


def row_pad(block, axis):
    short = -block.shape[axis] % TILE
    if not short:
        return block
    widths = [(0, 0)] * block.ndim
    widths[axis] = (0, short)
    return jnp.pad(block, widths)


def gather_weights(kernel_first, kernel_second, head_weight, action_embed):
    rows = kernel_first.shape[2]
    buckets = head_weight.shape[2]
    blocks = round_up(buckets, LANES) // LANES
    head = jnp.pad(head_weight[0], ((0, 0), (0, blocks * LANES - buckets)))
    head = head.reshape(rows, blocks, LANES).transpose(1, 0, 2)
    embed = jnp.pad(action_embed, ((0, TILE - 1), (0, LANES - rows)))
    packed = jnp.concatenate(
        [
            row_pad(kernel_first.astype(jnp.bfloat16).reshape(-1, LANES), 0),
            row_pad(kernel_second.astype(jnp.bfloat16).reshape(-1, LANES), 0),
            row_pad(head.astype(jnp.bfloat16).reshape(-1, LANES), 0),
            embed.astype(jnp.bfloat16),
        ]
    )
    mine = spread(packed, "dp")
    pair = (mine, swap_cores(mine))
    lines = [part[:, -TILE, :rows].reshape(CHANNELS) for part in pair]
    lower = lax.axis_index("mp") == 0
    embed_used = jnp.stack([jnp.where(lower, *lines), jnp.where(lower, *lines[::-1])])
    if rows != TILE:
        both = regroup(jnp.stack(pair), rows, blocks)
        pair = (both[0], both[1])
    return (pair, embed_used.astype(jnp.float32))


def regroup(everything, rows, blocks):
    cores, shards = everything.shape[:2]
    groups = CHANNELS // TILE
    parts = []
    begin = 0
    for taps in (9, 9, blocks):
        part = everything[:, :, begin : begin + taps * rows]
        begin += round_up(taps * rows, TILE)
        part = part.reshape(cores, groups, shards // groups, taps, rows, LANES)
        parts.append(part.transpose(0, 1, 3, 2, 4, 5).reshape(cores, groups, taps * TILE, LANES))
    parts.append(jnp.zeros((cores, groups, TILE, LANES), everything.dtype))
    return jnp.concatenate(parts, axis=2)


def ungroup(packed, rows, blocks, shards):
    cores, groups = packed.shape[:2]
    parts = []
    begin = 0
    for taps in (9, 9, blocks):
        part = packed[:, :, begin : begin + taps * TILE]
        begin += taps * TILE
        part = part.reshape(cores, groups, taps, shards // groups, rows, LANES)
        part = part.transpose(0, 1, 3, 2, 4, 5).reshape(cores, shards, taps * rows, LANES)
        parts.append(row_pad(part, 2))
    parts.append(jnp.repeat(packed[:, :, begin:], shards // groups, axis=1))
    return jnp.concatenate(parts, axis=2)


def scatter_grads(packed, rows, buckets):
    blocks = round_up(buckets, LANES) // LANES
    shards = lax.axis_size("dp")
    if rows != TILE:
        packed = ungroup(packed, rows, blocks, shards)
    arrived = swap_cores(packed[1])
    summed = packed[0].astype(jnp.float32) + arrived.astype(jnp.float32)
    summed = summed.astype(jnp.bfloat16)
    owned = lax.all_to_all(summed, "dp", 0, 0)
    total = jnp.sum(owned.astype(jnp.float32), axis=0)
    step = round_up(9 * rows, TILE)
    first = total[: 9 * rows].reshape(3, 3, rows, LANES)
    second = total[step : step + 9 * rows].reshape(3, 3, rows, LANES)
    head = total[2 * step : 2 * step + blocks * rows].reshape(blocks, rows, LANES)
    head = head.transpose(1, 0, 2).reshape(1, rows, blocks * LANES)[:, :, :buckets]
    embed = total[-TILE : CHANNELS // LANES - TILE].reshape(1, CHANNELS)
    embed = lax.dynamic_slice_in_dim(embed, lax.axis_index("dp") * rows, rows, 1)
    return (first, second, head, embed)


def nn(left, right):
    return jnp.dot(left, right, preferred_element_type=jnp.float32)


def nt(left, right):
    return lax.dot_general(left, right, (((1,), (1,)), ((), ())), preferred_element_type=jnp.float32)


def tn(left, right):
    return lax.dot_general(left, right, (((0,), (0,)), ((), ())), preferred_element_type=jnp.float32)


def window_kernel(
    spots,
    passes,
    values,
    rewards,
    place,
    mine,
    other,
    states,
    mask,
    embed,
    out,
    first,
    second,
    head,
    padded,
    fields,
    hiddens,
    taps,
    pres,
    sums,
    inners,
    branches,
    *,
    count,
    unroll,
    board,
    width,
    extent,
    buckets,
    blocks,
    total,
):
    cells = board * board
    base = 8
    scale = (9.0 * CHANNELS) ** (-0.5)
    cores = CHANNELS // LANES
    groups = CHANNELS // TILE
    spread_cols = blocks * LANES
    me = place[0]

    def fetch(core, group, at):
        rows = slice(at, at + TILE)
        return jnp.where(me == core, mine[group, rows, :], other[group, rows, :])

    for core in range(cores):
        lanes = slice(core * LANES, (core + 1) * LANES)
        for group in range(groups):
            for tap in range(9):
                at = tap * CHANNELS + group * TILE
                first[at : at + TILE, lanes] = fetch(core, group, tap * TILE)
                two = (9 + tap) * TILE
                second[at : at + TILE, lanes] = fetch(core, group, two)
    for which in range(2):
        for group in range(groups):
            for block in range(blocks):
                at = (18 + block) * TILE
                head[
                    which, group * TILE : (group + 1) * TILE, block * LANES : (block + 1) * LANES
                ] = fetch(which, group, at)
    padded[...] = jnp.zeros(padded.shape, jnp.float32)
    inside = jnp.broadcast_to(mask[...], (extent, CHANNELS)) > 0.5
    cell_at = lax.broadcasted_iota(jnp.int32, (extent, CHANNELS), 0)
    lane_at = lax.broadcasted_iota(jnp.int32, (8, spread_cols), 1)
    row_at = lax.broadcasted_iota(jnp.int32, (TILE, 1), 0)

    def lay_out(field, target, begin, flip):
        padded[base + width : base + width + extent, :] = field
        for tap in range(9):
            start = base + (tap // 3) * width + tap % 3 - 1
            slot = 8 - tap if flip else tap
            target[begin : begin + extent, slot * CHANNELS : (slot + 1) * CHANNELS] = padded[
                start : start + extent, :
            ].astype(jnp.bfloat16)

    def taps_nt(source, begin, kernel):
        result = None
        for tap in range(9):
            cols = slice(tap * CHANNELS, (tap + 1) * CHANNELS)
            part = nt(source[begin : begin + extent, cols], kernel[cols, :])
            result = part if result is None else result + part
        return result

    def grand(block):
        return jnp.sum(jnp.sum(block, axis=0, keepdims=True), axis=1, keepdims=True)

    pooled_rows = jnp.zeros((TILE, CHANNELS), jnp.float32)
    grad_rows = [jnp.zeros((TILE, spread_cols), jnp.float32) for _ in range(2)]
    factors = {}
    pulls = {}
    for n in range(count):
        state = states[n].astype(jnp.float32)
        for k in range(unroll):
            slot = k * count + n
            begin = slot * extent
            plane = cell_at == spots[n, k]
            extra = jnp.where(inside, passes[n, k].astype(jnp.float32) * embed[1:2, :], 0.0)
            mixed = state + jnp.where(plane, embed[0:1, :], 0.0) + extra
            lay_out(mixed, fields, begin, False)
            pre = scale * nn(fields[begin : begin + extent, :], first[...])
            pres[slot] = pre
            hidden = jnp.where(inside, pre * jax.nn.sigmoid(pre), 0.0)
            lay_out(hidden, hiddens, begin, False)
            branch = taps_nt(hiddens, begin, second)
            summed = jnp.where(inside, mixed + scale * branch, 0.0)
            sums[slot] = summed
            factor = lax.rsqrt(grand(summed * summed) / (cells * CHANNELS) + eps_norm)
            factors[slot] = factor
            state = summed * factor
            pooled = (jnp.sum(state, axis=0, keepdims=True) / cells).astype(jnp.bfloat16)
            pooled_rows = jnp.where(row_at == slot, pooled.astype(jnp.float32), pooled_rows)
            eight = jnp.broadcast_to(pooled.astype(jnp.float32), (8, CHANNELS)).astype(jnp.bfloat16)
            pull = jnp.zeros((8, CHANNELS), jnp.float32)
            for which, targets in enumerate((values, rewards)):
                raw = head_scale * nn(eight, head[which])
                squashed = jnp.tanh(raw / soft_cap)
                raised = jnp.where(lane_at < buckets, jnp.exp(soft_cap * squashed), 0.0)
                chances = raised / jnp.sum(raised, axis=1, keepdims=True)
                picked = jnp.where(lane_at == targets[n, k], 1.0, 0.0)
                logit_grad = (chances - picked) * (1.0 - squashed * squashed) / total
                rounded = logit_grad.astype(jnp.bfloat16)
                grad_rows[which] = jnp.where(
                    row_at == slot, rounded.astype(jnp.float32)[0:1, :], grad_rows[which]
                )
                pull = pull + nt(rounded, head[which])
            pulls[slot] = head_scale * pull[0:1, :]
    embed_grads = [jnp.zeros((1, CHANNELS), jnp.float32) for _ in range(2)]
    for n in range(count):
        carry = jnp.zeros((extent, CHANNELS), jnp.float32)
        for k in range(unroll - 1, -1, -1):
            slot = k * count + n
            begin = slot * extent
            factor = factors[slot]
            summed = sums[slot]
            state_grad = carry + jnp.where(inside, pulls[slot] / cells, 0.0)
            shared = grand(state_grad * summed) / (cells * CHANNELS)
            summed_grad = factor * state_grad - factor * factor * factor * summed * shared
            branches[begin : begin + extent, :] = summed_grad.astype(jnp.bfloat16)
            lay_out(summed_grad, taps, 0, True)
            hidden_grad = scale * nn(taps[...], second[...])
            pre = pres[slot]
            sig = jax.nn.sigmoid(pre)
            inner = jnp.where(inside, hidden_grad * (sig * (1.0 + pre * (1.0 - sig))), 0.0)
            inners[begin : begin + extent, :] = inner.astype(jnp.bfloat16)
            lay_out(inner, taps, 0, True)
            carry = jnp.where(inside, summed_grad + scale * taps_nt(taps, 0, first), 0.0)
            embed_grads[0] = embed_grads[0] + jnp.sum(
                jnp.where(cell_at == spots[n, k], carry, 0.0), axis=0, keepdims=True
            )
            embed_grads[1] = embed_grads[1] + passes[n, k].astype(jnp.float32) * jnp.sum(
                carry, axis=0, keepdims=True
            )
    turned_inner = inners[...].T
    turned_branch = branches[...].T
    for tap in range(9):
        cols = slice(tap * CHANNELS, (tap + 1) * CHANNELS)
        one = (scale * nn(turned_inner, fields[:, cols])).T.astype(jnp.bfloat16)
        two = (scale * nn(turned_branch, hiddens[:, cols])).astype(jnp.bfloat16)
        for core in range(cores):
            lanes = slice(core * LANES, (core + 1) * LANES)
            for group in range(groups):
                rows = slice(group * TILE, (group + 1) * TILE)
                out[me ^ core, group, tap * TILE : (tap + 1) * TILE, :] = one[rows, lanes]
                out[me ^ core, group, (9 + tap) * TILE : (10 + tap) * TILE, :] = two[rows, lanes]
    pooled_bf = pooled_rows.astype(jnp.bfloat16)
    for which in range(2):
        grown = head_scale * tn(pooled_bf, grad_rows[which].astype(jnp.bfloat16))
        grown = grown.astype(jnp.bfloat16)
        line = jnp.where(
            row_at == 0,
            embed_grads[which][:, :LANES],
            jnp.where(row_at == 1, embed_grads[which][:, LANES:], 0.0),
        ).astype(jnp.bfloat16)
        for group in range(groups):
            rows = slice(group * TILE, (group + 1) * TILE)
            for block in range(blocks):
                at = (18 + block) * TILE
                out[me ^ which, group, at : at + TILE, :] = grown[
                    rows, block * LANES : (block + 1) * LANES
                ]
            at = (18 + blocks) * TILE
            out[me ^ which, group, at : at + TILE, :] = line


def window(every, embed, states, moves, values, rewards, buckets, total):
    count, board = states.shape[:2]
    unroll = moves.shape[1]
    cells = board * board
    width = round_up(board + 1, 8)
    extent = round_up(board * width, TILE)
    blocks = round_up(buckets, LANES) // LANES
    states = jnp.pad(states, ((0, 0), (0, 0), (0, width - board), (0, 0)))
    states = states.reshape(count, board * width, CHANNELS)
    states = jnp.pad(states, ((0, 0), (0, extent - board * width), (0, 0)))
    passes = (moves == cells).astype(jnp.int32)
    spots = jnp.where(moves == cells, -1, moves // board * width + moves % board)
    at = jnp.arange(extent)
    mask = ((at % width < board) & (at // width < board)).astype(jnp.float32)[:, None]
    deep = count * unroll * extent
    body = functools.partial(
        window_kernel,
        count=count,
        unroll=unroll,
        board=board,
        width=width,
        extent=extent,
        buckets=buckets,
        blocks=blocks,
        total=total,
    )
    place = lax.axis_index("mp").reshape(1)
    smem = pl.BlockSpec(memory_space=pltpu.SMEM)
    vmem = pl.BlockSpec(memory_space=pltpu.VMEM)
    return pl.pallas_call(
        body,
        out_shape=jax.ShapeDtypeStruct((2,) + every[0].shape, jnp.bfloat16),
        in_specs=[smem] * 5 + [vmem] * 5,
        out_specs=vmem,
        scratch_shapes=[
            pltpu.VMEM((9 * CHANNELS, CHANNELS), jnp.bfloat16),
            pltpu.VMEM((9 * CHANNELS, CHANNELS), jnp.bfloat16),
            pltpu.VMEM((2, CHANNELS, blocks * LANES), jnp.bfloat16),
            pltpu.VMEM((extent + 2 * width + 16, CHANNELS), jnp.float32),
            pltpu.VMEM((deep, 9 * CHANNELS), jnp.bfloat16),
            pltpu.VMEM((deep, 9 * CHANNELS), jnp.bfloat16),
            pltpu.VMEM((extent, 9 * CHANNELS), jnp.bfloat16),
            pltpu.VMEM((count * unroll, extent, CHANNELS), jnp.float32),
            pltpu.VMEM((count * unroll, extent, CHANNELS), jnp.float32),
            pltpu.VMEM((deep, CHANNELS), jnp.bfloat16),
            pltpu.VMEM((deep, CHANNELS), jnp.bfloat16),
        ],
        compiler_params=pltpu.CompilerParams(vmem_limit_bytes=56 * 1024 * 1024),
    )(spots, passes, values, rewards, place, *every, states, mask, embed)


def local(
    hidden_state,
    actions,
    value_target,
    reward_target,
    kernel_first,
    kernel_second,
    head_weight,
    action_embed,
    first_mean,
    first_square,
    second_mean,
    second_square,
    head_mean,
    head_square,
    embed_mean,
    embed_square,
):
    total = hidden_state.shape[0] * lax.axis_size("dp")
    rows = kernel_first.shape[2]
    buckets = head_weight.shape[2]
    every, embed = gather_weights(kernel_first, kernel_second, head_weight, action_embed)
    count = hidden_state.shape[0] // lax.axis_size("mp")
    begin = lax.axis_index("mp") * count
    states = lax.dynamic_slice_in_dim(hidden_state, begin, count, 0)
    moves = lax.dynamic_slice_in_dim(actions, begin, count, 0)
    values = lax.dynamic_slice_in_dim(value_target, begin, count, 0)
    rewards = lax.dynamic_slice_in_dim(reward_target, begin, count, 0)
    packed = window(every, embed, states, moves, values, rewards, buckets, total)
    first_grad, second_grad, head_grad, embed_grad = scatter_grads(packed, rows, buckets)
    first_new, first_mean_new, first_square_new = adam_update(
        kernel_first, first_grad, first_mean, first_square
    )
    second_new, second_mean_new, second_square_new = adam_update(
        kernel_second, second_grad, second_mean, second_square
    )
    head_new, head_mean_new, head_square_new = adam_update(
        head_weight, head_grad, head_mean, head_square
    )
    embed_new, embed_mean_new, embed_square_new = adam_update(
        action_embed, embed_grad, embed_mean, embed_square
    )
    return (
        first_new,
        second_new,
        head_new,
        embed_new,
        first_mean_new,
        first_square_new,
        second_mean_new,
        second_square_new,
        head_mean_new,
        head_square_new,
        embed_mean_new,
        embed_square_new,
        first_grad,
        second_grad,
        head_grad,
        embed_grad,
    )


def solution(mesh):
    placed = (
        P("dp", None, None, None),
        P("dp", None),
        P("dp", None),
        P("dp", None),
        P(None, None, "dp", "mp"),
        P(None, None, "dp", "mp"),
        P("mp", "dp", None),
        P("mp", "dp"),
        P(None, None, "dp", "mp"),
        P(None, None, "dp", "mp"),
        P(None, None, "dp", "mp"),
        P(None, None, "dp", "mp"),
        P("mp", "dp", None),
        P("mp", "dp", None),
        P("mp", "dp"),
        P("mp", "dp"),
    )
    return jax.shard_map(
        local,
        mesh=mesh,
        in_specs=placed,
        out_specs=(
            P(None, None, "dp", "mp"),
            P(None, None, "dp", "mp"),
            P("mp", "dp", None),
            P("mp", "dp"),
            P(None, None, "dp", "mp"),
            P(None, None, "dp", "mp"),
            P(None, None, "dp", "mp"),
            P(None, None, "dp", "mp"),
            P("mp", "dp", None),
            P("mp", "dp", None),
            P("mp", "dp"),
            P("mp", "dp"),
            P(None, None, "dp", "mp"),
            P(None, None, "dp", "mp"),
            P("mp", "dp", None),
            P("mp", "dp"),
        ),
        check_vma=False,
    )
```
